32 devices in a mesh: grp: 2 (over y), row: 8 (over z, x), col: 1, ch: 2 (over core).
Axes of the slice: x: 2, y: 2, z: 4, core: 2. Of those that a mesh axis runs over, the one named last changes fastest.
Arguments:
- pair_act: bfloat16 [128, 256, 128], P('ch', ('grp', 'row'), 'col'), parts along dimension 1, may hold values from -48 to 48
- in_gain: float32 [128], P('ch'), may hold values from 0.1 to 1.9
- left_proj: bfloat16 [128, 128], P(None, 'ch'), may hold values from -0.5 to 0.5
- left_gate: bfloat16 [128, 128], P(None, 'ch'), may hold values from -0.5 to 0.5
- right_proj: bfloat16 [128, 128], P(None, 'ch'), may hold values from -0.5 to 0.5
- right_gate: bfloat16 [128, 128], P(None, 'ch'), may hold values from -0.5 to 0.5
- out_gate: bfloat16 [128, 128], P(None, 'ch'), may hold values from -0.5 to 0.5
- out_gain: float32 [128], P('ch'), may hold values from 0.1 to 1.9
- out_proj: bfloat16 [128, 128], P(None, 'ch'), may hold values from -0.5 to 0.5
Outputs:
- update: bfloat16 [128, 256, 128], P('ch', ('grp', 'row'), 'col'), parts along dimension 1
The draws below stay inside these ranges and needn't reach their ends.
There are 2 independent parts, one for each index of `grp`. The reference program is written for one: setup_inputs(seed, part) draws one part's arguments, and reference() takes and returns one part's arrays. A program takes and returns all parts, laid end to end along the dimension named above; an argument that names none is the same for every part. Nothing has to cross between parts.
All inputs are finite; a program needn't handle non-finite values.
Results may differ from the reference program's by a relative error of at most 0.0085.
Values may be sent and summed in bfloat16 or wider, within the bound.
No kernel may reach another device: no remote copies, remote signals or barrier semaphores. Data moves between devices by JAX's collectives and lax.ppermute only.
A program may use at most 64 MiB of HBM per device.

```python
import jax
import jax.numpy as jnp
from jax import lax

C = 128
HID = 128
RES = 128


def draw_pair_act(key, part):
    keys = jax.random.split(jax.random.fold_in(key, 11), 4)
    base = jnp.clip(jax.random.normal(keys[0], (C, RES, RES), jnp.float32), -5.0, 5.0)
    channel_scale = jnp.exp(jax.random.uniform(keys[1], (C, 1, 1), jnp.float32, jnp.log(0.3), jnp.log(3.0)))
    site_scale = jnp.exp(jax.random.uniform(keys[2], (1, RES, RES), jnp.float32, jnp.log(0.3), jnp.log(3.0)))
    offset = 0.5 * jnp.clip(jax.random.normal(keys[3], (1, RES, RES), jnp.float32), -3.0, 3.0)
    return (base * channel_scale * site_scale + offset).astype(jnp.bfloat16)


def level_of(stream_key, extent, shards, low, largest):
    level = 1.0
    for position, parts in shards:
        heights = jax.random.uniform(jax.random.fold_in(jax.random.fold_in(stream_key, 6), position), (parts,), jnp.float32, low / len(shards), largest / len(shards))
        level = level * jnp.repeat(jnp.exp(heights), extent[position] // parts).reshape((-1,) + (1,) * (len(extent) - 1 - position))
    return level


def normal_values(own_key, extent, deviation, limit, shards=(), kind=jnp.bfloat16):
    entries = jax.random.normal(own_key, extent, jnp.float32) * deviation
    if len(shards) > 0:
        entries = level_of(own_key, extent, shards, -0.22, 0.18) * entries
    return jnp.clip(entries, min=-limit, max=limit).astype(kind)


def setup_inputs(seed: int = 0, part: int = 0) -> dict:
    key_list = jax.random.split(jax.random.key(seed), 10)
    part_splits = jax.random.split(jax.random.fold_in(key_list[9], part), 10)
    return {
        "pair_act": draw_pair_act(jax.random.fold_in(jax.random.fold_in(key_list[9], part), 71), part),
        "in_gain": jnp.clip(1.0 + 0.18 * jax.random.normal(key_list[1], (C,), jnp.float32), 0.1, 1.9),
        "left_proj": normal_values(key_list[2], (C, HID), C ** -0.5, 0.5, ((1, 2),)),
        "left_gate": normal_values(key_list[3], (C, HID), C ** -0.5, 0.5, ((1, 2),)),
        "right_proj": normal_values(key_list[4], (C, HID), C ** -0.5, 0.5, ((1, 2),)),
        "right_gate": normal_values(key_list[5], (C, HID), C ** -0.5, 0.5, ((1, 2),)),
        "out_gate": normal_values(key_list[6], (C, C), C ** -0.5, 0.5, ((1, 2),)),
        "out_gain": jnp.clip(1.0 + 0.18 * jax.random.normal(key_list[7], (HID,), jnp.float32), 0.1, 1.9),
        "out_proj": normal_values(key_list[8], (HID, C), HID ** -0.5, 0.5, ((1, 2),)),
    }


def layer_norm(values, gain):
    average = lax.optimization_barrier(jnp.mean(values, axis=0, keepdims=True))
    spread = lax.optimization_barrier(jnp.mean(jnp.square(values - average), axis=0, keepdims=True))
    return (values - average) * lax.rsqrt(spread + 1e-05) * gain[:, None, None]

def reference(pair_act, in_gain, left_proj, left_gate, right_proj, right_gate, out_gate, out_gain, out_proj):
    pair_float = pair_act.astype(jnp.float32)
    normed = layer_norm(pair_float, in_gain).astype(jnp.bfloat16)
    normed_float = normed.astype(jnp.float32)

    def lift_by(matrix):
        return jnp.einsum('cxy,ch->hxy', normed_float, matrix.astype(jnp.float32))
    left_edge = (jax.nn.sigmoid(lift_by(left_gate)) * lift_by(left_proj)).astype(jnp.bfloat16)
    right_edge = (jax.nn.sigmoid(lift_by(right_gate)) * lift_by(right_proj)).astype(jnp.bfloat16)
    gate_map = jax.nn.sigmoid(lift_by(out_gate))
    tri_sum = jnp.einsum('hki,hkj->hij', left_edge.astype(jnp.float32), right_edge.astype(jnp.float32))
    mid_norm = layer_norm(tri_sum, out_gain).astype(jnp.bfloat16)
    projected = jnp.einsum('hxy,hc->cxy', mid_norm.astype(jnp.float32), out_proj.astype(jnp.float32))
    return (gate_map * projected).astype(jnp.bfloat16)
```

```python
import functools

import jax
import jax.numpy as jnp
from jax import lax
from jax.experimental import pallas as pl
from jax.experimental.pallas import tpu as pltpu
from jax.sharding import PartitionSpec as P


F32 = jnp.float32
BF16 = jnp.bfloat16
EPS = 1e-05


def call(body, out_shapes, scratch, flops, *operands):
    return pl.pallas_call(
        body,
        out_shape=out_shapes,
        scratch_shapes=scratch,
        in_specs=[pl.BlockSpec(memory_space=pltpu.VMEM)] * len(operands),
        out_specs=jax.tree.map(lambda _: pl.BlockSpec(memory_space=pltpu.VMEM), out_shapes),
        cost_estimate=pl.CostEstimate(flops=flops, bytes_accessed=1 << 20, transcendentals=0),
    )(*operands)


def channel_parts(value):
    count = lax.axis_size("ch")
    return [value] + [
        lax.ppermute(value, "ch", [((i + s) % count, i) for i in range(count)])
        for s in range(1, count)
    ]


def row_exchange(blocks):
    count = lax.axis_size("row")
    return [blocks[0]] + [
        lax.ppermute(blocks[d], "row", [(i, i ^ d) for i in range(count)])
        for d in range(1, count)
    ]


def part_start(s, count, size):
    return pl.multiple_of(((lax.axis_index("ch") + s) % count) * size, size)


def fill_gains(gains, gain_scr):
    count = len(gains)
    size = gains[0].shape[0]
    lanes = gain_scr.shape[1]
    for s in range(count):
        line = jnp.broadcast_to(gains[s][...].reshape(1, size), (lanes, size))
        gain_scr[pl.ds(part_start(s, count, size), size), :] = line.T


def normalise(values, gain):
    average = jnp.mean(values, axis=0, keepdims=True)
    centred = values - average
    spread = jnp.mean(centred * centred, axis=0, keepdims=True)
    return (centred * lax.rsqrt(spread + EPS) * gain).astype(BF16)


def edges_body(count, row_count, *refs):
    acts, gains = refs[:count], refs[count : 2 * count]
    lp, lg, rp, rg = refs[2 * count : 2 * count + 4]
    outs = refs[2 * count + 4 : 2 * count + 4 + row_count]
    normed_ref, flat, gain_scr, weights = refs[2 * count + 4 + row_count :]
    size, rows, cols = acts[0].shape
    channels = size * count
    hidden = lp.shape[0]
    group = hidden // row_count
    me = lax.axis_index("row")
    fill_gains(gains, gain_scr)
    for s in range(count):
        flat[pl.ds(part_start(s, count, size) * rows, size * rows), :] = (
            acts[s][...].astype(F32).reshape(size * rows, cols)
        )
    for n, w in enumerate((lp, rp, lg, rg)):
        weights[n] = w[...].astype(F32)
    pieces = []
    for pair in ((0, 1), (2, 3)):
        for d in range(row_count):
            start = pl.multiple_of((me ^ d) * group, group)
            for n in pair:
                pieces.append(weights[n, pl.ds(start, group), :])
    stacked = jnp.concatenate(pieces, axis=0).astype(BF16)
    half = 2 * hidden
    gain = gain_scr[...]
    for x in range(rows):
        normed = normalise(flat[pl.ds(x, channels, stride=rows), :], gain)
        normed_ref[x] = normed
        lifted = jnp.dot(stacked, normed, preferred_element_type=F32)
        edges = (jax.nn.sigmoid(lifted[half:]) * lifted[:half]).astype(BF16)
        for d in range(row_count):
            outs[d][x] = edges[2 * group * d : 2 * group * (d + 1)]


def gate_body(normed, weight, out):
    for x in range(normed.shape[0]):
        out[x] = jax.nn.sigmoid(jnp.dot(weight[...], normed[x], preferred_element_type=F32))


def triangle_body(row_count, separate, *refs):
    blocks = refs[:row_count]
    refs = refs[row_count:]
    if separate:
        left_ref, refs = refs[0], refs[1:]
    outs, refs = refs[:row_count], refs[row_count:]
    flat, tri = refs[:2]
    rows, pair, cols = blocks[0].shape
    group = pair // 2
    depth = rows * row_count
    me = lax.axis_index("row")
    for d in range(row_count):
        flat[pl.ds(d * rows * pair, rows * pair), :] = (
            blocks[d][...].astype(F32).reshape(rows * pair, cols)
        )
    for h in range(group):
        right = flat[pl.ds(group + h, depth, stride=pair), :].astype(BF16)
        if separate:
            left = left_ref[h]
        else:
            left = flat[pl.ds(h, depth, stride=pair), :].astype(BF16)
        tri[h] = lax.dot_general(
            left, right, (((0,), (0,)), ((), ())), preferred_element_type=F32
        )
    for d in range(row_count):
        start = pl.multiple_of((me ^ d) * rows, rows)
        outs[d][...] = tri[:, pl.ds(start, rows), :].astype(BF16)


def update_body(count, row_count, *refs):
    tris, gains = refs[:count], refs[count : 2 * count]
    gate, weight, out, flat, gain_scr, wide = refs[2 * count :]
    size, rows, cols = tris[0].shape
    group = size // row_count
    channels = size * count
    me = lax.axis_index("row")
    fill_gains(gains, gain_scr)
    for s in range(count):
        base = part_start(s, count, size)
        for d in range(row_count):
            start = pl.multiple_of((base + (me ^ d) * group) * rows, group * rows)
            flat[pl.ds(start, group * rows), :] = (
                tris[s][group * d : group * (d + 1)].astype(F32).reshape(group * rows, cols)
            )
    gain = gain_scr[...]
    outs = weight.shape[0]
    for x in range(rows):
        mid = normalise(flat[pl.ds(x, channels, stride=rows), :], gain)
        projected = jnp.dot(weight[...], mid, preferred_element_type=F32)
        wide[pl.ds(x, outs, stride=rows), :] = gate[x] * projected
    out[...] = wide[...].reshape(outs, rows, cols).astype(BF16)


def per_device(
    pair_act, in_gain, left_proj, left_gate, right_proj, right_gate, out_gate, out_gain, out_proj
):
    size, rows, cols = pair_act.shape
    count = lax.axis_size("ch")
    row_count = lax.axis_size("row")
    col_count = lax.axis_size("col")
    channels = size * count
    hidden = left_proj.shape[1]
    hidden_all = hidden * count
    group = hidden // row_count
    outs = out_proj.shape[1]
    shape = jax.ShapeDtypeStruct

    acts = channel_parts(pair_act)
    in_gains = channel_parts(in_gain)
    *edges, normed = call(
        functools.partial(edges_body, count, row_count),
        [shape((rows, 2 * group, cols), BF16)] * row_count + [shape((rows, channels, cols), BF16)],
        [
            pltpu.VMEM((channels * rows, cols), F32),
            pltpu.VMEM((channels, cols), F32),
            pltpu.VMEM((4, hidden, channels), F32),
        ],
        8 * hidden * channels * rows * cols,
        *acts, *in_gains, left_proj.T, left_gate.T, right_proj.T, right_gate.T,
    )
    arrived = row_exchange(edges)
    out_gains = channel_parts(out_gain)
    gate_map = call(
        gate_body, shape((rows, outs, cols), F32), [], 2 * outs * channels * rows * cols,
        normed, out_gate.T,
    )
    depth = rows * row_count
    separate = col_count > 1
    extra = ()
    if separate:
        left = jnp.concatenate(arrived, axis=0)[:, :group].transpose(1, 0, 2)
        extra = (lax.all_gather(left, "col", axis=2, tiled=True),)
    tri_blocks = call(
        functools.partial(triangle_body, row_count, separate),
        [shape((group, rows, cols), BF16)] * row_count,
        [
            pltpu.VMEM((depth * 2 * group, cols), F32),
            pltpu.VMEM((group, cols * col_count, cols), F32),
        ],
        2 * group * depth * cols * cols * col_count,
        *arrived, *extra,
    )
    tri = jnp.concatenate(row_exchange(tri_blocks), axis=0)
    tris = channel_parts(tri)
    return call(
        functools.partial(update_body, count, row_count),
        shape((outs, rows, cols), BF16),
        [
            pltpu.VMEM((hidden_all * rows, cols), F32),
            pltpu.VMEM((hidden_all, cols), F32),
            pltpu.VMEM((outs * rows, cols), F32),
        ],
        2 * hidden_all * outs * rows * cols,
        *tris, *out_gains, gate_map, out_proj.T,
    )


def solution(mesh):
    return jax.shard_map(
        per_device,
        mesh=mesh,
        in_specs=(
            P("ch", ("grp", "row"), "col"),
            P("ch"),
            P(None, "ch"),
            P(None, "ch"),
            P(None, "ch"),
            P(None, "ch"),
            P(None, "ch"),
            P("ch"),
            P(None, "ch"),
        ),
        out_specs=P("ch", ("grp", "row"), "col"),
        check_vma=False,
    )
```

```python
import functools

import jax
import jax.numpy as jnp
from jax import lax
from jax.experimental import pallas as pl
from jax.experimental.pallas import tpu as pltpu
from jax.sharding import PartitionSpec as P


F32 = jnp.float32
BF16 = jnp.bfloat16
EPS = 1e-05


def near(value):
    return pltpu.with_memory_space_constraint(value, pltpu.VMEM)


def call(body, out_shapes, scratch, flops, *operands):
    return pl.pallas_call(
        body,
        out_shape=out_shapes,
        scratch_shapes=scratch,
        in_specs=[pl.BlockSpec(memory_space=pltpu.VMEM)] * len(operands),
        out_specs=jax.tree.map(lambda _: pl.BlockSpec(memory_space=pltpu.VMEM), out_shapes),
        cost_estimate=pl.CostEstimate(flops=flops, bytes_accessed=1 << 20, transcendentals=0),
    )(*operands)


def channel_parts(value):
    count = lax.axis_size("ch")
    return [value] + [
        near(lax.ppermute(value, "ch", [((i + s) % count, i) for i in range(count)]))
        for s in range(1, count)
    ]


def row_exchange(blocks):
    count = lax.axis_size("row")
    arrived = [blocks[0]]
    for d in range(1, count):
        arrived.append(lax.ppermute(blocks[d], "row", [(i, i ^ d) for i in range(count)]))
    return arrived


def part_start(s, count, size):
    return pl.multiple_of(((lax.axis_index("ch") + s) % count) * size, size)


def fill_gains(gains, gain_scr):
    count = len(gains)
    size = gains[0].shape[0]
    lanes = gain_scr.shape[1]
    for s in range(count):
        line = jnp.broadcast_to(gains[s][...].reshape(1, size), (lanes, size))
        gain_scr[pl.ds(part_start(s, count, size), size), :] = line.T


def normalise(values, gain):
    average = jnp.mean(values, axis=0, keepdims=True)
    centred = values - average
    spread = jnp.mean(centred * centred, axis=0, keepdims=True)
    return (centred * lax.rsqrt(spread + EPS) * gain).astype(BF16)


def edges_body(count, row_count, *refs):
    acts, gains = refs[:count], refs[count : 2 * count]
    lp, lg, rp, rg = refs[2 * count : 2 * count + 4]
    outs = refs[2 * count + 4 : 2 * count + 4 + row_count]
    normed_ref, flat, gain_scr, weights = refs[2 * count + 4 + row_count :]
    size, rows, cols = acts[0].shape
    channels = size * count
    hidden = lp.shape[0]
    group = hidden // row_count
    me = lax.axis_index("row")
    fill_gains(gains, gain_scr)
    for s in range(count):
        flat[pl.ds(part_start(s, count, size) * rows, size * rows), :] = (
            acts[s][...].astype(F32).reshape(size * rows, cols)
        )
    for n, w in enumerate((lp, rp, lg, rg)):
        weights[n] = w[...].astype(F32)
    pieces = []
    for pair in ((0, 1), (2, 3)):
        for d in range(row_count):
            start = pl.multiple_of((me ^ d) * group, group)
            for n in pair:
                pieces.append(weights[n, pl.ds(start, group), :])
    stacked = jnp.concatenate(pieces, axis=0).astype(BF16)
    half = 2 * hidden
    gain = gain_scr[...]
    for x in range(rows):
        normed = normalise(flat[pl.ds(x, channels, stride=rows), :], gain)
        normed_ref[x] = normed
        lifted = jnp.dot(stacked, normed, preferred_element_type=F32)
        edges = (jax.nn.sigmoid(lifted[half:]) * lifted[:half]).astype(BF16)
        for d in range(row_count):
            outs[d][x] = edges[2 * group * d : 2 * group * (d + 1)]


def gate_body(normed, weight, out):
    for x in range(normed.shape[0]):
        out[x] = jax.nn.sigmoid(jnp.dot(weight[...], normed[x], preferred_element_type=F32))


def triangle_body(row_count, separate, *refs):
    blocks = refs[:row_count]
    refs = refs[row_count:]
    if separate:
        left_ref, refs = refs[0], refs[1:]
    outs, refs = refs[:row_count], refs[row_count:]
    flat, tri = refs[:2]
    rows, pair, cols = blocks[0].shape
    group = pair // 2
    depth = rows * row_count
    me = lax.axis_index("row")
    for d in range(row_count):
        flat[pl.ds(d * rows * pair, rows * pair), :] = (
            blocks[d][...].astype(F32).reshape(rows * pair, cols)
        )
    for h in range(group):
        right = flat[pl.ds(group + h, depth, stride=pair), :].astype(BF16)
        if separate:
            left = left_ref[h]
        else:
            left = flat[pl.ds(h, depth, stride=pair), :].astype(BF16)
        tri[h] = lax.dot_general(
            left, right, (((0,), (0,)), ((), ())), preferred_element_type=F32
        )
    for d in range(row_count):
        start = pl.multiple_of((me ^ d) * rows, rows)
        outs[d][...] = tri[:, pl.ds(start, rows), :].astype(BF16)


def update_body(count, row_count, *refs):
    tris, gains = refs[:count], refs[count : 2 * count]
    gate, weight, out, flat, gain_scr, wide = refs[2 * count :]
    size, rows, cols = tris[0].shape
    group = size // row_count
    channels = size * count
    me = lax.axis_index("row")
    fill_gains(gains, gain_scr)
    for s in range(count):
        base = part_start(s, count, size)
        for d in range(row_count):
            start = pl.multiple_of((base + (me ^ d) * group) * rows, group * rows)
            flat[pl.ds(start, group * rows), :] = (
                tris[s][group * d : group * (d + 1)].astype(F32).reshape(group * rows, cols)
            )
    gain = gain_scr[...]
    outs = weight.shape[0]
    for x in range(rows):
        mid = normalise(flat[pl.ds(x, channels, stride=rows), :], gain)
        projected = jnp.dot(weight[...], mid, preferred_element_type=F32)
        wide[pl.ds(x, outs, stride=rows), :] = gate[x] * projected
    out[...] = wide[...].reshape(outs, rows, cols).astype(BF16)


def steps(
    pair_act, in_gain, left_proj, left_gate, right_proj, right_gate, out_gate, out_gain, out_proj
):
    size, rows, cols = pair_act.shape
    count = lax.axis_size("ch")
    row_count = lax.axis_size("row")
    col_count = lax.axis_size("col")
    channels = size * count
    hidden = left_proj.shape[1]
    hidden_all = hidden * count
    group = hidden // row_count
    outs = out_proj.shape[1]
    shape = pltpu.VMEM

    acts = channel_parts(pair_act)
    in_gains = channel_parts(in_gain)
    out_gains = channel_parts(out_gain)
    *edges, normed = call(
        functools.partial(edges_body, count, row_count),
        [shape((rows, 2 * group, cols), BF16)] * row_count + [shape((rows, channels, cols), BF16)],
        [
            pltpu.VMEM((channels * rows, cols), F32),
            pltpu.VMEM((channels, cols), F32),
            pltpu.VMEM((4, hidden, channels), F32),
        ],
        8 * hidden * channels * rows * cols,
        *acts, *in_gains, left_proj.T, left_gate.T, right_proj.T, right_gate.T,
    )
    arrived = row_exchange(edges)
    gate_map = call(
        gate_body, shape((rows, outs, cols), F32), [], 2 * outs * channels * rows * cols,
        near(normed), out_gate.T,
    )
    depth = rows * row_count
    separate = col_count > 1
    extra = ()
    if separate:
        left = jnp.concatenate(arrived, axis=0)[:, :group].transpose(1, 0, 2)
        extra = (lax.all_gather(left, "col", axis=2, tiled=True),)
    tri_blocks = call(
        functools.partial(triangle_body, row_count, separate),
        [shape((group, rows, cols), BF16)] * row_count,
        [
            pltpu.VMEM((depth * 2 * group, cols), F32),
            pltpu.VMEM((group, cols * col_count, cols), F32),
        ],
        2 * group * depth * cols * cols * col_count,
        *map(near, arrived), *extra,
    )
    tri = jnp.concatenate(row_exchange(tri_blocks), axis=0)
    tris = channel_parts(tri)
    return call(
        functools.partial(update_body, count, row_count),
        jax.ShapeDtypeStruct((outs, rows, cols), BF16),
        [
            pltpu.VMEM((hidden_all * rows, cols), F32),
            pltpu.VMEM((hidden_all, cols), F32),
            pltpu.VMEM((outs * rows, cols), F32),
        ],
        2 * hidden_all * outs * rows * cols,
        near(tri), *tris[1:], *out_gains, near(gate_map), out_proj.T,
    )


def solution(mesh):
    return jax.shard_map(
        steps,
        mesh=mesh,
        in_specs=(
            P("ch", ("grp", "row"), "col"),
            P("ch"),
            P(None, "ch"),
            P(None, "ch"),
            P(None, "ch"),
            P(None, "ch"),
            P(None, "ch"),
            P("ch"),
            P(None, "ch"),
        ),
        out_specs=P("ch", ("grp", "row"), "col"),
        check_vma=False,
    )
```

```python
import functools

import jax
import jax.numpy as jnp
from jax import lax
from jax.experimental import pallas as pl
from jax.experimental.pallas import tpu as pltpu
from jax.sharding import PartitionSpec as P


F32 = jnp.float32
BF16 = jnp.bfloat16
EPS = 1e-05


def near(value):
    return pltpu.with_memory_space_constraint(value, pltpu.VMEM)


def call(body, out_shapes, scratch, flops, *operands):
    return pl.pallas_call(
        body,
        out_shape=out_shapes,
        scratch_shapes=scratch,
        in_specs=[pl.BlockSpec(memory_space=pltpu.VMEM)] * len(operands),
        out_specs=jax.tree.map(lambda _: pl.BlockSpec(memory_space=pltpu.VMEM), out_shapes),
        cost_estimate=pl.CostEstimate(flops=flops, bytes_accessed=1 << 20, transcendentals=0),
    )(*operands)


def channel_parts(value):
    count = lax.axis_size("ch")
    return [value] + [
        near(lax.ppermute(value, "ch", [((i + s) % count, i) for i in range(count)]))
        for s in range(1, count)
    ]


def row_exchange(blocks):
    count = lax.axis_size("row")
    arrived = [blocks[0]]
    for d in range(1, count):
        arrived.append(lax.ppermute(blocks[d], "row", [(i, i ^ d) for i in range(count)]))
    return arrived


def fill_gains(gains, gain_scr):
    size = gains[0].shape[0]
    lanes = gain_scr.shape[1]
    for s, gain in enumerate(gains):
        line = jnp.broadcast_to(gain[...].reshape(1, size), (lanes, size))
        gain_scr[s * size : (s + 1) * size, :] = line.T


def own_first(weight):
    channels = weight.shape[1]
    own = lax.axis_index("ch") * (channels // lax.axis_size("ch"))
    return pltpu.roll(weight[...].astype(F32), (channels - own) % channels, 1)


def normalise(values, gain):
    average = jnp.mean(values, axis=0, keepdims=True)
    centred = values - average
    spread = jnp.mean(centred * centred, axis=0, keepdims=True)
    return (centred * lax.rsqrt(spread + EPS) * gain).astype(BF16)


def prepare_body(row_count, act, lp, lg, rp, rg, flat, stacked, weights):
    size, rows, cols = act.shape
    hidden = lp.shape[0]
    group = hidden // row_count
    me = lax.axis_index("row")
    for n, w in enumerate((lp, rp, lg, rg)):
        weights[n] = own_first(w)
    pieces = []
    for pair in ((0, 1), (2, 3)):
        for d in range(row_count):
            start = pl.multiple_of((me ^ d) * group, group)
            for n in pair:
                pieces.append(weights[n, pl.ds(start, group), :])
    stacked[...] = jnp.concatenate(pieces, axis=0).astype(BF16)
    flat[...] = act[...].astype(F32).reshape(size * rows, cols)


def edges_body(count, row_count, *refs):
    own, stacked, refs = refs[0], refs[1], refs[2:]
    others, gains, refs = refs[: count - 1], refs[count - 1 : 2 * count - 1], refs[2 * count - 1 :]
    outs, refs = refs[:row_count], refs[row_count:]
    normed_ref, flat, gain_scr = refs
    rows, pair, cols = outs[0].shape
    size = own.shape[0] // rows
    half = stacked.shape[0] // 2
    fill_gains(gains, gain_scr)
    for s, other in enumerate(others):
        flat[s * size * rows : (s + 1) * size * rows, :] = (
            other[...].astype(F32).reshape(size * rows, cols)
        )
    gain = gain_scr[...]
    for x in range(rows):
        values = jnp.concatenate(
            [own[pl.ds(x, size, stride=rows), :]]
            + [flat[pl.ds(x, (count - 1) * size, stride=rows), :]] * (count > 1),
            axis=0,
        )
        normed = normalise(values, gain)
        normed_ref[x] = normed
        lifted = jnp.dot(stacked[...], normed, preferred_element_type=F32)
        edges = (jax.nn.sigmoid(lifted[half:]) * lifted[:half]).astype(BF16)
        for d in range(row_count):
            outs[d][x] = edges[pair * d : pair * (d + 1)]


def gate_body(count, *refs):
    normed, gate_weight, proj_weight = refs[:3]
    gains, (gate, weight, gain_col) = refs[3 : 3 + count], refs[3 + count :]
    fill_gains(gains, gain_col)
    weight[...] = own_first(proj_weight).astype(BF16)
    rotated = own_first(gate_weight).astype(BF16)
    for x in range(normed.shape[0]):
        gate[x] = jax.nn.sigmoid(jnp.dot(rotated, normed[x], preferred_element_type=F32))


def triangle_body(row_count, separate, *refs):
    blocks = refs[:row_count]
    refs = refs[row_count:]
    if separate:
        left_ref, refs = refs[0], refs[1:]
    outs, refs = refs[:row_count], refs[row_count:]
    flat, tri = refs[:2]
    rows, pair, cols = blocks[0].shape
    group = pair // 2
    depth = rows * row_count
    me = lax.axis_index("row")
    for d in range(row_count):
        flat[pl.ds(d * rows * pair, rows * pair), :] = (
            blocks[d][...].astype(F32).reshape(rows * pair, cols)
        )
    for h in range(group):
        right = flat[pl.ds(group + h, depth, stride=pair), :].astype(BF16)
        if separate:
            left = left_ref[h]
        else:
            left = flat[pl.ds(h, depth, stride=pair), :].astype(BF16)
        tri[h] = lax.dot_general(
            left, right, (((0,), (0,)), ((), ())), preferred_element_type=F32
        )
    for d in range(row_count):
        start = pl.multiple_of((me ^ d) * rows, rows)
        outs[d][...] = tri[:, pl.ds(start, rows), :].astype(BF16)


def update_body(count, row_count, *refs):
    tris = refs[:count]
    gate, weight, gain_col, out, flat, wide = refs[count:]
    size, rows, cols = tris[0].shape
    group = size // row_count
    channels = size * count
    me = lax.axis_index("row")
    for s in range(count):
        for d in range(row_count):
            start = pl.multiple_of((s * size + (me ^ d) * group) * rows, group * rows)
            flat[pl.ds(start, group * rows), :] = (
                tris[s][group * d : group * (d + 1)].astype(F32).reshape(group * rows, cols)
            )
    gain = gain_col[...]
    outs = weight.shape[0]
    for x in range(rows):
        mid = normalise(flat[pl.ds(x, channels, stride=rows), :], gain)
        projected = jnp.dot(weight[...], mid, preferred_element_type=F32)
        wide[pl.ds(x, outs, stride=rows), :] = gate[x] * projected
    out[...] = wide[...].reshape(outs, rows, cols).astype(BF16)


def steps(
    pair_act, in_gain, left_proj, left_gate, right_proj, right_gate, out_gate, out_gain, out_proj
):
    size, rows, cols = pair_act.shape
    count = lax.axis_size("ch")
    row_count = lax.axis_size("row")
    col_count = lax.axis_size("col")
    channels = size * count
    hidden = left_proj.shape[1]
    hidden_all = hidden * count
    group = hidden // row_count
    outs = out_proj.shape[1]
    shape = pltpu.VMEM

    acts = channel_parts(pair_act)
    in_gains = channel_parts(in_gain)
    out_gains = channel_parts(out_gain)
    flat, stacked = call(
        functools.partial(prepare_body, row_count),
        [shape((size * rows, cols), F32), shape((4 * hidden, channels), BF16)],
        [pltpu.VMEM((4, hidden, channels), F32)],
        1 << 20,
        pair_act, left_proj.T, left_gate.T, right_proj.T, right_gate.T,
    )
    *edges, normed = call(
        functools.partial(edges_body, count, row_count),
        [shape((rows, 2 * group, cols), BF16)] * row_count
        + [shape((rows, channels, cols), BF16)],
        [
            pltpu.VMEM((max(count - 1, 1) * size * rows, cols), F32),
            pltpu.VMEM((channels, cols), F32),
        ],
        8 * hidden * channels * rows * cols,
        near(flat), near(stacked), *acts[1:], *in_gains,
    )
    arrived = row_exchange(edges)
    late = call(
        functools.partial(gate_body, count),
        [
            shape((rows, outs, cols), F32),
            shape((outs, hidden_all), BF16),
            shape((hidden_all, cols), F32),
        ],
        [],
        2 * outs * channels * rows * cols,
        near(normed), out_gate.T, out_proj.T, *out_gains,
    )
    depth = rows * row_count
    separate = col_count > 1
    extra = ()
    if separate:
        left = jnp.concatenate(arrived, axis=0)[:, :group].transpose(1, 0, 2)
        extra = (lax.all_gather(left, "col", axis=2, tiled=True),)
    tri_blocks = call(
        functools.partial(triangle_body, row_count, separate),
        [shape((group, rows, cols), BF16)] * row_count,
        [
            pltpu.VMEM((depth * 2 * group, cols), F32),
            pltpu.VMEM((group, cols * col_count, cols), F32),
        ],
        2 * group * depth * cols * cols * col_count,
        *map(near, arrived), *extra,
    )
    tri = jnp.concatenate(row_exchange(tri_blocks), axis=0)
    tris = channel_parts(tri)
    return call(
        functools.partial(update_body, count, row_count),
        jax.ShapeDtypeStruct((outs, rows, cols), BF16),
        [
            pltpu.VMEM((hidden_all * rows, cols), F32),
            pltpu.VMEM((outs * rows, cols), F32),
        ],
        2 * hidden_all * outs * rows * cols,
        near(tri), *tris[1:], *map(near, late),
    )


def solution(mesh):
    return jax.shard_map(
        steps,
        mesh=mesh,
        in_specs=(
            P("ch", ("grp", "row"), "col"),
            P("ch"),
            P(None, "ch"),
            P(None, "ch"),
            P(None, "ch"),
            P(None, "ch"),
            P(None, "ch"),
            P("ch"),
            P(None, "ch"),
        ),
        out_specs=P("ch", ("grp", "row"), "col"),
        check_vma=False,
    )
```
